64 devices in a mesh: dp: 4 (over x, y), ep: 16 (over z, core).
Axes of the slice: x: 2, y: 2, z: 8, core: 2. Of those that a mesh axis runs over, the one named last changes fastest.
The devices are a block of a 4x4x8 slice.
Arguments:
- h0: bfloat16 [64, 128, 2048], P(('dp', 'ep')), parts along dimension 0
- idx: int32 [64, 128, 8], P(('dp', 'ep')), parts along dimension 0
- slot: int32 [64, 128, 8], P(('dp', 'ep')), parts along dimension 0
- norm_attn: bfloat16 [2048], replicated
- wq: bfloat16 [2048, 4096], replicated
- wk: bfloat16 [2048, 512], replicated
- wv: bfloat16 [2048, 512], replicated
- wo: bfloat16 [4096, 2048], replicated
- norm_ffn: bfloat16 [2048], replicated
- w1: bfloat16 [2048, 6144], replicated
- w3: bfloat16 [2048, 6144], replicated
- w2: bfloat16 [6144, 2048], replicated
- norm_moe: bfloat16 [2048], replicated
- wr: bfloat16 [2048, 128], replicated
- ue1: bfloat16 [128, 2048, 768], P('ep')
- ue3: bfloat16 [128, 2048, 768], P('ep')
- ue2: bfloat16 [128, 768, 2048], P('ep')
Outputs:
- output: bfloat16 [64, 128, 2048], P(('dp', 'ep')), parts along dimension 0
There are 4 independent parts. The reference program is written for one: setup_inputs(seed, part) draws one part's arguments, and reference() takes and returns one part's arrays. A program takes and returns all parts, laid end to end along the dimension named above; an argument that names none is the same for every part.
All inputs are finite; a program needn't handle non-finite values.
Results may differ from the reference program's by a relative error of at most 0.0127771.
Values are sent between devices in bfloat16 or wider.
A program may use at most 768 MiB of HBM per device.

```python
import jax
import jax.numpy as jnp
from jax import lax

D = 2048
HEADS = 32
KV_HEADS = 4
HEAD = 128
FF = 6144
EXPERTS = 128
TOP = 8
FE = 768
SEQS_DEV = 1
SEQ = 128
EP = 16

TOKENS = SEQS_DEV * SEQ
CAP = 2 * TOKENS * TOP // EXPERTS
EPS = 1e-6
ROPE_BASE = 10000.0


def _w(key, shape, fan_in, scale=1.0):
    return (scale * fan_in ** -0.5 * jax.random.normal(key, shape, jnp.float32)).astype(jnp.bfloat16)


def _perms(key, count, size):
    return jax.vmap(lambda k: jax.random.permutation(k, size))(jax.random.split(key, count))


def setup_inputs(seed: int = 0, part: int = 0) -> dict:
    key = jax.random.PRNGKey(seed)
    ks = jax.random.split(key, 14)
    kp = jax.random.split(jax.random.fold_in(key, part), 4)
    kd = jax.random.split(jax.random.fold_in(jax.random.fold_in(key, part), 7), 4)
    avg = TOKENS * TOP // EXPERTS
    c = jnp.arange(TOKENS * TOP).reshape(TOKENS, TOP)
    half = TOKENS * TOP // 2
    low = c < half
    e0 = jnp.where(low, c % EXPERTS, (c - half) % (EXPERTS // 2))
    s0 = jnp.where(low, c // EXPERTS, avg // 2 + (c - half) // (EXPERTS // 2))
    shift = jax.random.randint(kd[2], (EP, EXPERTS), 0, CAP)
    tperm = jnp.broadcast_to(_perms(kd[3], EP, TOKENS)[:, :, None], (EP, TOKENS, TOP))
    idx = jnp.take_along_axis(jnp.broadcast_to(e0, (EP, TOKENS, TOP)), tperm, axis=1)
    slot = jnp.take_along_axis((s0[None] + shift[:, e0]) % CAP, tperm, axis=1)
    rshape = (EP * SEQS_DEV, SEQ, TOP)

    def nrm(k):
        return (1.0 + 0.2 * jax.random.normal(k, (D,), jnp.float32)).astype(jnp.bfloat16)

    return {
        'h0': jax.random.normal(kp[0], (EP * SEQS_DEV, SEQ, D), jnp.float32).astype(jnp.bfloat16),
        'idx': idx.reshape(rshape).astype(jnp.int32),
        'slot': slot.reshape(rshape).astype(jnp.int32),
        'norm_attn': nrm(ks[0]),
        'wq': _w(ks[1], (D, HEADS * HEAD), D),
        'wk': _w(ks[2], (D, KV_HEADS * HEAD), D),
        'wv': _w(ks[3], (D, KV_HEADS * HEAD), D),
        'wo': _w(ks[4], (HEADS * HEAD, D), HEADS * HEAD, 2.0),
        'norm_ffn': nrm(ks[5]),
        'w1': _w(ks[6], (D, FF), D),
        'w3': _w(ks[7], (D, FF), D),
        'w2': _w(ks[8], (FF, D), FF, 2.0),
        'norm_moe': nrm(ks[9]),
        'wr': _w(ks[10], (D, EXPERTS), D, 2.0),
        'ue1': _w(ks[11], (EXPERTS, D, FE), D),
        'ue3': _w(ks[12], (EXPERTS, D, FE), D),
        'ue2': _w(ks[13], (EXPERTS, FE, D), FE, 2.0),
    }


def _rms(x, w):
    xf = x.astype(jnp.float32)
    r = lax.rsqrt(jnp.mean(xf * xf, axis=-1, keepdims=True) + EPS)
    return (xf * r * w.astype(jnp.float32)).astype(jnp.bfloat16)


def _rope(x, cos, sin):
    h = HEAD // 2
    x1 = x[..., :h]
    x2 = x[..., h:]
    return jnp.concatenate([x1 * cos - x2 * sin, x2 * cos + x1 * sin], axis=-1)


def _dense_seq(h, na, wq, wk, wv, wo, nf, w1, w3, w2):
    f32 = jnp.float32
    bf = jnp.bfloat16
    pos = jnp.arange(SEQ).astype(f32)
    inv = ROPE_BASE ** (-2.0 * jnp.arange(HEAD // 2).astype(f32) / HEAD)
    ang = pos[:, None] * inv[None, :]
    cos = jnp.cos(ang)[:, None, :]
    sin = jnp.sin(ang)[:, None, :]
    x = _rms(h, na)
    q = _rope(jnp.dot(x, wq, preferred_element_type=f32).reshape(SEQ, HEADS, HEAD), cos, sin).astype(bf)
    k = _rope(jnp.dot(x, wk, preferred_element_type=f32).reshape(SEQ, KV_HEADS, HEAD), cos, sin).astype(bf)
    v = jnp.dot(x, wv, preferred_element_type=f32).astype(bf).reshape(SEQ, KV_HEADS, HEAD)
    q = q.reshape(SEQ, KV_HEADS, HEADS // KV_HEADS, HEAD)
    s = jnp.einsum('qgrd,kgd->grqk', q.astype(f32), k.astype(f32)) * HEAD ** -0.5
    causal = jnp.arange(SEQ)[:, None] >= jnp.arange(SEQ)[None, :]
    s = jnp.where(causal, s, -jnp.inf)
    p = jax.nn.softmax(s, axis=-1).astype(bf)
    o = jnp.einsum('grqk,kgd->qgrd', p.astype(f32), v.astype(f32)).astype(bf).reshape(SEQ, HEADS * HEAD)
    a = (h.astype(f32) + jnp.dot(o, wo, preferred_element_type=f32)).astype(bf)
    z = _rms(a, nf)
    hid = (jax.nn.silu(jnp.dot(z, w1, preferred_element_type=f32)) * jnp.dot(z, w3, preferred_element_type=f32)).astype(bf)
    return a.astype(f32) + jnp.dot(hid, w2, preferred_element_type=f32)


def reference(h0, idx, slot, norm_attn, wq, wk, wv, wo, norm_ffn, w1, w3, w2, norm_moe, wr, ue1, ue3, ue2):
    f32 = jnp.float32
    bf = jnp.bfloat16
    n = EP * TOKENS
    ix = idx.reshape(n, TOP)
    sl = slot.reshape(n, TOP)
    u = _rms(h0.reshape(n, D), norm_moe)
    logits = jnp.dot(u, wr, preferred_element_type=f32)
    g = jax.nn.softmax(jnp.take_along_axis(logits, ix, axis=1), axis=-1)
    rows = jnp.broadcast_to(jnp.arange(n, dtype=jnp.int32)[:, None], (n, TOP))
    src = rows // TOKENS
    tok = jnp.full((EP, EXPERTS, CAP), n, jnp.int32).at[src, ix, sl].set(rows)
    gb = jnp.zeros((EP, EXPERTS, CAP), f32).at[src, ix, sl].set(g)
    tok = tok.transpose(1, 0, 2).reshape(EXPERTS, EP * CAP)
    x = jnp.take(u, tok, axis=0, mode='fill', fill_value=0)

    def expert(args):
        xe, e1, e3, e2 = args
        hid = (jax.nn.silu(jnp.dot(xe, e1, preferred_element_type=f32)) * jnp.dot(xe, e3, preferred_element_type=f32)).astype(bf)
        return jnp.dot(hid, e2, preferred_element_type=f32).astype(bf)

    y = lax.map(expert, (x, ue1, ue3, ue2))
    gw = gb.transpose(1, 0, 2).reshape(EXPERTS, EP * CAP, 1)
    m = jnp.zeros((n, D), f32).at[tok.reshape(-1)].add((gw * y.astype(f32)).reshape(-1, D), mode='drop')
    dense = lax.map(lambda hs: _dense_seq(hs, norm_attn, wq, wk, wv, wo, norm_ffn, w1, w3, w2), h0)
    return (dense + m.reshape(EP * SEQS_DEV, SEQ, D)).astype(bf)
```

```python
import jax
import jax.numpy as jnp
from jax import lax
from jax.sharding import PartitionSpec as P

HEAD = 128
EPS = 1e-6
ROPE_BASE = 10000.0


def _rms(x, w):
    xf = x.astype(jnp.float32)
    r = lax.rsqrt(jnp.mean(xf * xf, axis=-1, keepdims=True) + EPS)
    return (xf * r * w.astype(jnp.float32)).astype(jnp.bfloat16)


def _rope(x, cos, sin):
    h = HEAD // 2
    x1, x2 = x[..., :h], x[..., h:]
    return jnp.concatenate([x1 * cos - x2 * sin, x2 * cos + x1 * sin], axis=-1)


def _dense(h0, na, wq, wk, wv, wo, nf, w1, w3, w2):
    f32, bf = jnp.float32, jnp.bfloat16
    b, s, d = h0.shape
    nh = wq.shape[1] // HEAD
    nkvv = wk.shape[1] // HEAD
    pos = jnp.arange(s).astype(f32)
    inv = ROPE_BASE ** (-2.0 * jnp.arange(HEAD // 2).astype(f32) / HEAD)
    ang = pos[:, None] * inv[None, :]
    cos, sin = jnp.cos(ang)[:, None, :], jnp.sin(ang)[:, None, :]
    x = _rms(h0, na).reshape(b * s, d)
    q = _rope(jnp.dot(x, wq, preferred_element_type=f32).reshape(b, s, nh, HEAD), cos, sin).astype(bf)
    k = _rope(jnp.dot(x, wk, preferred_element_type=f32).reshape(b, s, nkvv, HEAD), cos, sin).astype(bf)
    v = jnp.dot(x, wv, preferred_element_type=f32).astype(bf).reshape(b, s, nkvv, HEAD)
    q = q.reshape(b, s, nkvv, nh // nkvv, HEAD)
    sc = jnp.einsum('bqgrd,bkgd->bgrqk', q, k, preferred_element_type=f32) * HEAD ** -0.5
    causal = jnp.arange(s)[:, None] >= jnp.arange(s)[None, :]
    sc = jnp.where(causal, sc, -jnp.inf)
    p = jax.nn.softmax(sc, axis=-1).astype(bf)
    o = jnp.einsum('bgrqk,bkgd->bqgrd', p, v, preferred_element_type=f32).astype(bf).reshape(b * s, nh * HEAD)
    a = (h0.reshape(b * s, d).astype(f32) + jnp.dot(o, wo, preferred_element_type=f32)).astype(bf)
    z = _rms(a, nf)
    hid = (jax.nn.silu(jnp.dot(z, w1, preferred_element_type=f32)) * jnp.dot(z, w3, preferred_element_type=f32)).astype(bf)
    return a.astype(f32) + jnp.dot(hid, w2, preferred_element_type=f32)


def _route(h0, nm, wr, idx):
    d = h0.shape[-1]
    k = idx.shape[-1]
    u = _rms(h0, nm).reshape(-1, d)
    logits = jnp.dot(u, wr, preferred_element_type=jnp.float32)
    hot = idx.reshape(-1, k)[:, :, None] == jnp.arange(wr.shape[1])[None, None, :]
    g = jax.nn.softmax(jnp.sum(jnp.where(hot, logits[:, None, :], 0.0), -1), axis=-1)
    return u, g


def _split3(g):
    bf, f32 = jnp.bfloat16, jnp.float32
    hi = lax.reduce_precision(g, 8, 7)
    r = g - hi
    mid = lax.reduce_precision(r, 8, 7)
    lo = r - mid
    return hi.astype(bf), mid.astype(bf), lo.astype(bf)


def solution(mesh):
    G = mesh.shape['ep']

    def local(h0, idx, slot, na, wq, wk, wv, wo, nf, w1, w3, w2, nm, wr, ue1, ue3, ue2):
        f32, bf = jnp.float32, jnp.bfloat16
        b, s, d = h0.shape
        t = b * s
        k = idx.shape[-1]
        el = ue1.shape[0]
        e = el * G
        cap = 2 * t * k // e
        u, g = _route(h0, nm, wr, idx)
        key = (idx * cap + slot).reshape(t, k)
        ua = lax.all_gather(u, 'ep', axis=0, tiled=False)
        ka = lax.all_gather(key, 'ep', axis=0, tiled=False)
        ga = lax.all_gather(g, 'ep', axis=0, tiled=False)
        n = el * cap
        base = lax.axis_index('ep') * n
        rows = base + jnp.arange(n)
        hot = ka[:, :, :, None] == rows[None, None, None, :]
        sel = jnp.any(hot, axis=2).astype(bf)
        gm = jnp.sum(jnp.where(hot, ga[..., None], 0.0), axis=2)
        x = jnp.einsum('gtn,gtd->gnd', sel, ua, preferred_element_type=f32).astype(bf)
        x = x.reshape(G, el, cap, d).transpose(1, 0, 2, 3).reshape(el, G * cap, d)
        h1 = jnp.einsum('ecd,edf->ecf', x, ue1, preferred_element_type=f32)
        h3 = jnp.einsum('ecd,edf->ecf', x, ue3, preferred_element_type=f32)
        hid = (jax.nn.silu(h1) * h3).astype(bf)
        y = jnp.einsum('ecf,efd->ecd', hid, ue2, preferred_element_type=f32).astype(bf)
        y = y.reshape(el, G, cap, d).transpose(1, 0, 2, 3).reshape(G, n, d)
        part = sum(jnp.einsum('gtn,gnd->gtd', w, y, preferred_element_type=f32) for w in _split3(gm))
        m = lax.psum_scatter(part, 'ep', scatter_dimension=0, tiled=False)
        dense = _dense(h0, na, wq, wk, wv, wo, nf, w1, w3, w2)
        return (dense + m).astype(bf).reshape(b, s, d)

    rows_spec = P(('dp', 'ep'))
    in_specs = (rows_spec,) * 3 + (P(),) * 11 + (P('ep'),) * 3
    return jax.shard_map(local, mesh=mesh, in_specs=in_specs, out_specs=rows_spec, check_vma=False)
```

```python
import functools

import jax
import jax.numpy as jnp
import numpy as np
from jax import lax
from jax.experimental import pallas as pl
from jax.experimental.pallas import tpu as pltpu
from jax.sharding import PartitionSpec as P

HEAD = 128
EPS = 1e-6
ROPE_BASE = 10000.0
TN = 256
NS = 4
VMEM_LIMIT = 66_500_000
MESH = pl.DeviceIdType.MESH
F32, BF = jnp.float32, jnp.bfloat16


def _rms_rows(xf, w):
    r = lax.rsqrt(jnp.mean(xf * xf, axis=-1, keepdims=True) + EPS)
    return (xf * r * w).astype(BF)


def _silu(x):
    return x * jax.nn.sigmoid(x)


def _div(x, n):
    return x // n if isinstance(x, int) else lax.div(x, n)


def _rem(x, n):
    return x % n if isinstance(x, int) else lax.rem(x, n)


def _dot(a, b):
    return jnp.dot(a, b, preferred_element_type=F32)


class Phase:
    def __init__(self, n, copies):
        self.n, self.copies, self.start = n, copies, 0


def _kernel(Z, T, D, NQ, NK, FF, EL, FE, CAP,
            h0, keyt, idxt, na, nf, nm, wr, cosr, sinr,
            wq, wk, wv, wo, w1, w3, w2, ue1, ue3, ue2,
            out,
            ubuf, kg, x, hid, ys, yr, g3, rb, ms, mr, wbuf, xn, qkv, o, a, fh, f,
            wsem, own_s, own_r, ag_s, ag_r, kg_s, kg_r, dd_s, dd_r, y_s, y_r, rs_s, rs_r, m_s, m_r):
    ep = lax.axis_index("ep")
    z = _div(ep, 2)
    k = _rem(ep, 2)
    ok = 1 - k
    RC = T // 16
    HC = RC // 2
    NC = D // TN
    NCH = NC // 2
    NM = 4 * HC - 2 if Z == 8 else None
    assert Z == 8 and HC == 4 and NCH == 4
    NSL = EL * CAP

    def dev(zz, kk):
        return {"ep": zz * 2 + kk}

    right, left = _rem(z + 1, Z), _rem(z + Z - 1, Z)
    nbr = (right, left)

    def rcopy(src, dst, s, r, zz, kk):
        return pltpu.make_async_remote_copy(src_ref=src, dst_ref=dst, send_sem=s, recv_sem=r,
                                            device_id=dev(zz, kk), device_id_type=MESH)

    def cols(i):
        return pl.ds(i * TN if isinstance(i, int) else pl.multiple_of(i * TN, TN), TN)

    def wslot(slot, lo, n):
        return wbuf.at[slot, pl.ds(lo, n)]

    nq2, nk2 = NQ // (2 * TN), NK // (2 * TN)

    def qkv_copies(i, slot):
        res = []
        for h in range(2):
            for cond, src, off in ((i < nq2, wq, 0), ((i >= nq2) & (i < nq2 + nk2), wk, nq2),
                                   (i >= nq2 + nk2, wv, nq2 + nk2)):
                res.append((cond, lambda src=src, off=off, h=h: pltpu.make_async_copy(
                    src.at[:, cols(2 * (i - off) + h)], wslot(slot, h * D, D), wsem.at[slot, h])))
        return res

    def wo_copies(i, slot):
        return [(None, lambda: pltpu.make_async_copy(wo.at[:, cols(i)], wslot(slot, 0, NQ), wsem.at[slot, 0]))]

    def w13_copies(i0):
        def go(i, slot):
            return [(None, lambda: pltpu.make_async_copy(w1.at[:, cols(i + i0)], wslot(slot, 0, D), wsem.at[slot, 0])),
                    (None, lambda: pltpu.make_async_copy(w3.at[:, cols(i + i0)], wslot(slot, D, D), wsem.at[slot, 1]))]
        return go

    def w2_copies(i, slot):
        return [(None, lambda: pltpu.make_async_copy(w2.at[:, cols(i)], wslot(slot, 0, FF), wsem.at[slot, 0]))]

    NJ = FE // TN

    def e1_copies(i, slot):
        e, j = _div(i, NJ), _rem(i, NJ)
        return [(None, lambda: pltpu.make_async_copy(ue1.at[e, :, cols(j)], wslot(slot, 0, D), wsem.at[slot, 0])),
                (None, lambda: pltpu.make_async_copy(ue3.at[e, :, cols(j)], wslot(slot, D, D), wsem.at[slot, 1]))]

    def e2_col(i):
        q = _div(i, 2)
        c = _rem(q, 2) * 2 + _div(q, 2)
        half = jnp.where(_rem(i, 2) == 0, ok, k)
        return half, c

    def e2_copies(i, slot):
        half, c = e2_col(i)
        return [(None, lambda e=e: pltpu.make_async_copy(
            ue2.at[e, :, cols(half * NCH + c)], wslot(slot, e * FE, FE), wsem.at[slot, e])) for e in range(EL)]

    n13 = FF // TN
    n13a = n13 // 4
    ph_qkv = Phase(nq2 + 2 * nk2, qkv_copies)
    ph_wo = Phase(D // TN, wo_copies)
    ph_13a = Phase(n13a, w13_copies(0))
    ph_e1 = [Phase(EL * NJ, e1_copies), Phase(EL * NJ, e1_copies)]
    ph_e2 = [Phase(NC, e2_copies), Phase(NC, e2_copies)]
    ph_13b = Phase(n13 - n13a, w13_copies(n13a))
    ph_2 = Phase(D // TN, w2_copies)
    order = [ph_qkv, ph_wo, ph_13a, ph_e1[0], ph_e2[0], ph_e1[1], ph_e2[1], ph_13b, ph_2]
    total = 0
    for q, ph in enumerate(order):
        ph.start, ph.pos = total, q
        total += ph.n

    def do(copies, act):
        for cond, mk in copies:
            if cond is None:
                act(mk())
            else:
                pl.when(cond)(lambda mk=mk: act(mk()))

    def issue(t, phases):
        slot = _rem(t, NS)
        for ph in phases:
            def go(ph=ph):
                do(ph.copies(t - ph.start, slot), lambda c: c.start())
            pl.when((t >= ph.start) & (t < ph.start + ph.n))(go)

    def run(ph, body, events=None):
        nxt = order[ph.pos:ph.pos + 2]

        def it(i, _):
            t = ph.start + i
            slot = _rem(t, NS)
            do(ph.copies(i, slot), lambda c: c.wait())
            body(i, slot)
            issue(t + NS, nxt)
            if events is not None:
                events(i)
            return 0

        lax.fori_loop(0, ph.n, it, 0)

    def at(i, start, stride, count, fn, e0):
        n = _div(i - start, stride)
        pl.when((i >= start) & (_rem(i - start, stride) == 0) & (n < count))(lambda: fn(e0 + n))

    def ag_desc(p, dirn, i):
        d = _div(i, 4)
        c = _rem(i + 2 * dirn, 4)
        org = _rem(z - d + Z, Z) if dirn == 0 else _rem(z + d, Z)
        blk = ubuf.at[p, org, k * HC + c]
        return rcopy(blk, blk, ag_s.at[p, dirn, i], ag_r.at[p, dirn, i], nbr[dirn], k)

    def kg_desc(p, dirn, d):
        org = _rem(z - d + Z, Z) if dirn == 0 else _rem(z + d, Z)
        blk = kg.at[p, org]
        return rcopy(blk, blk, kg_s.at[p, dirn, d], kg_r.at[p, dirn, d], nbr[dirn], k)

    def dd_desc(p, dirn, i):
        d = _div(i, 4) + 1
        c = _rem(i + 2 * dirn, 4)
        org = _rem(z - d + Z, Z) if dirn == 0 else _rem(z + d, Z)
        blk = ubuf.at[p, org, k * HC + c]
        return rcopy(blk, blk, dd_s.at[p, dirn, i], dd_r.at[p, dirn, i], z, ok)

    def own_descs(p):
        return (rcopy(ubuf.at[p, z], ubuf.at[p, z], own_s.at[0], own_r.at[0], z, ok),
                rcopy(kg.at[p, z], kg.at[p, z], own_s.at[1], own_r.at[1], z, ok))

    NKG = (4, 3)

    def ag_begin(p):
        @pl.when(k != p)
        def _():
            for c in own_descs(p):
                c.wait_recv()
        for i in range(4):
            for dirn in range(2):
                ag_desc(p, dirn, i).start()
                if i == 0:
                    kg_desc(p, dirn, 0).start()

    def ag_event(p):
        def ev(i):
            for dirn in range(2):
                ag_desc(p, dirn, i).wait_recv()
                pl.when(i < 10)(lambda: ag_desc(p, dirn, i + 4).start())
                dd_desc(p, dirn, i).start()
                q = _div(i, 4)

                @pl.when((_rem(i, 4) == 0) & (q < NKG[dirn]))
                def _():
                    kg_desc(p, dirn, q).wait_recv()
                    pl.when(q + 1 < NKG[dirn])(lambda: kg_desc(p, dirn, q + 1).start())
        return ev

    def ag_drain(p):
        for dirn in range(2):
            @pl.loop(0, 14)
            def _(i):
                dd_desc(p, dirn, i).wait_recv()

    def key_hits(p, zs, j, base, n):
        keys = kg[p, zs, j:j + 1, :].astype(jnp.int32)
        return keys == base + lax.broadcasted_iota(jnp.int32, (n, T), 0)

    def select(p, zs):
        base = ep * NSL
        s = jnp.zeros((NSL, T), jnp.bool_)
        s = key_hits(p, zs, 0, base, NSL)
        for j in range(1, 8):
            s = s | key_hits(p, zs, j, base, NSL)
        s = jnp.where(s, 1.0, 0.0).astype(BF)
        for n in range(D // 512):
            u = ubuf[p, zs, :, :, n * 512:(n + 1) * 512].reshape(T, 512)
            xs = _dot(s, u).astype(BF)
            for e in range(EL):
                x[e, zs, :, n * 512:(n + 1) * 512] = xs[e * CAP:(e + 1) * CAP]

    def gates(p, zs):
        parts = []
        for kk in (k, ok):
            base = (z * 2 + kk) * NSL
            gt = jnp.zeros((NSL, T), F32)
            for j in range(8):
                gt = gt + jnp.where(key_hits(p, zs, j, base, NSL), kg[p, zs, 8 + j:9 + j, :], 0.0)
            parts.append(gt.T)
        for h, gt in enumerate(parts):
            hi = gt.astype(BF)
            r = gt - hi.astype(F32)
            mid = r.astype(BF)
            lo = (r - mid.astype(F32)).astype(BF)
            for q, v in enumerate((hi, mid, lo)):
                g3[p, zs, q * T:(q + 1) * T, h * NSL:(h + 1) * NSL] = v

    def combine(p, zd, c):
        yy = jnp.concatenate([ys[p, k, c, zd], yr[p, c, zd]], axis=0)
        r = _dot(g3[p, zd], yy)
        return r[:T] + (r[T:2 * T] + r[2 * T:])

    def rs_desc(p, dirn, i):
        return rcopy(rb.at[p, dirn, i], rb.at[p, dirn, i + 4], rs_s.at[p, dirn, i], rs_r.at[p, dirn, i],
                     nbr[dirn], k)

    def rs_event(p):
        def ev(i):
            j = i + 2
            d = 4 - _div(j, 4)
            for dirn in range(2):
                c = _rem(j + 2 - 2 * dirn, 4)
                zd = _rem(z + d, Z) if dirn == 0 else _rem(z - d + Z, Z)
                part = combine(p, zd, c)

                @pl.when(i >= 4)
                def _():
                    rs_desc(p, dirn, i - 4).wait_recv()
                    rb[p, dirn, i] = rb[p, dirn, i] + part

                @pl.when(i < 4)
                def _():
                    rb[p, dirn, i] = part
            for dirn in range(2):
                rs_desc(p, dirn, i).start()
        return ev

    def m_desc(p):
        return rcopy(ms.at[p], mr, m_s.at[0], m_r.at[0], z, ok)

    def rs_final(p):
        @pl.loop(0, 4)
        def _(s):
            c = _rem(s + 2, 4)
            rs_desc(p, 0, 10 + s).wait_recv()
            ms[p, c] = combine(p, z, c) + rb[p, 0, 14 + s]

        @pl.loop(0, 4)
        def _(c):
            rs_desc(p, 1, 10 + c).wait_recv()
            ms[p, c] = ms[p, c] + rb[p, 1, 14 + c]

        pl.when(k != p)(lambda: m_desc(p).start())

    def y_desc(p, c):
        return rcopy(ys.at[p, ok, c], yr.at[p, c], y_s.at[p, c], y_r.at[p, c], z, ok)

    def qkv_body(i, slot):
        last = i >= nq2 + nk2
        cs = jnp.where(last, 1.0, cosr[...])
        sn = jnp.where(last, 0.0, sinr[...])
        for h in range(2):
            r = _dot(xn[...], wbuf[slot, h * D:(h + 1) * D])
            parts = []
            for b in range(TN // HEAD):
                v = r[:, b * HEAD:(b + 1) * HEAD]
                parts.append(v * cs + pltpu.roll(v, HEAD // 2, 1) * sn)
            qkv[:, cols(2 * i + h)] = jnp.concatenate(parts, axis=1).astype(BF)

    nkv = NK // HEAD
    rep = NQ // NK

    def attn(g):
        def hd(i):
            return pl.ds(pl.multiple_of(i * HEAD, HEAD), HEAD)
        kk = qkv[:, hd(NQ // HEAD + g)]
        vv = qkv[:, hd(NQ // HEAD + nkv + g)]
        causal = lax.broadcasted_iota(jnp.int32, (T, T), 0) >= lax.broadcasted_iota(jnp.int32, (T, T), 1)
        for hh in range(rep):
            qh = qkv[:, hd(g * rep + hh)]
            s = lax.dot_general(qh, kk, (((1,), (1,)), ((), ())), preferred_element_type=F32) * HEAD ** -0.5
            s = jnp.where(causal, s, -jnp.inf)
            e = jnp.exp(s - jnp.max(s, axis=-1, keepdims=True))
            pr = (e / jnp.sum(e, axis=-1, keepdims=True)).astype(BF)
            o[:, hd(g * rep + hh)] = _dot(pr, vv).astype(BF)

    def wo_body(i, slot):
        r = _dot(o[...], wbuf[slot, :NQ])
        a[:, cols(i)] = (h0[:, cols(i)].astype(F32) + r).astype(BF)

    def w13_body(i0):
        def body(i, slot):
            h1 = _dot(xn[...], wbuf[slot, :D])
            h3 = _dot(xn[...], wbuf[slot, D:2 * D])
            fh[:, cols(i + i0)] = (_silu(h1) * h3).astype(BF)
        return body

    def w2_body(i, slot):
        f[:, cols(i)] = _dot(fh[...], wbuf[slot, :FF])

    def e1_body(i, slot):
        e, j = _div(i, NJ), _rem(i, NJ)
        xe = x[e].reshape(Z * CAP, D)
        h1 = _dot(xe, wbuf[slot, :D])
        h3 = _dot(xe, wbuf[slot, D:2 * D])
        hid[e, :, cols(j)] = (_silu(h1) * h3).astype(BF)

    def e2_body(p):
        def body(i, slot):
            half, c = e2_col(i)
            for e in range(EL):
                r = _dot(hid[e], wbuf[slot, e * FE:(e + 1) * FE]).astype(BF)
                for zs in range(Z):
                    ys[p, half, c, zs, e * CAP:(e + 1) * CAP, :] = r[zs * CAP:(zs + 1) * CAP]
            pl.when(_rem(i, 2) == 0)(lambda: y_desc(p, c).start())
        return body

    barrier = pltpu.get_barrier_semaphore()
    for zz, kk in ((right, k), (left, k), (z, ok)):
        pl.semaphore_signal(barrier, inc=1, device_id=dev(zz, kk), device_id_type=MESH)

    for t in range(NS):
        issue(t, [ph_qkv])

    @pl.loop(0, RC)
    def _(r):
        rows = pl.ds(pl.multiple_of(r * 16, 16), 16)
        hf = h0[rows, :].astype(F32)
        ubuf[k, z, r] = _rms_rows(hf, nm[...].astype(F32))
        xn[rows, :] = _rms_rows(hf, na[...].astype(F32))

    lt = _dot(ubuf[k, z].reshape(T, D), wr[...]).T
    rows = []
    for j in range(8):
        hit = lax.broadcasted_iota(jnp.int32, lt.shape, 0) == idxt[j:j + 1, :]
        rows.append(jnp.sum(jnp.where(hit, lt, 0.0), axis=0, keepdims=True))
    sel = jnp.concatenate(rows, axis=0)
    ex = jnp.exp(sel - jnp.max(sel, axis=0, keepdims=True))
    kg[k, z, 0:8, :] = keyt[...].astype(F32)
    kg[k, z, 8:16, :] = ex / jnp.sum(ex, axis=0, keepdims=True)

    pl.semaphore_wait(barrier, 3)
    for p in range(2):
        @pl.when(k == p)
        def _():
            for c in own_descs(p):
                c.start()
    ag_begin(0)

    ag0, ag1 = ag_event(0), ag_event(1)
    rs0, rs1 = rs_event(0), rs_event(1)

    run(ph_qkv, qkv_body, lambda i: at(i, 3, 2, 3, ag0, 0))

    @pl.loop(0, nkv)
    def _(g):
        attn(g)
        ag0(3 + g)

    run(ph_wo, wo_body, lambda i: at(i, 1, 2, 4, ag0, 7))
    ag_begin(1)

    @pl.loop(0, RC)
    def _(r):
        rows = pl.ds(pl.multiple_of(r * 16, 16), 16)
        xn[rows, :] = _rms_rows(a[rows, :].astype(F32), nf[...].astype(F32))

    run(ph_13a, w13_body(0), lambda i: at(i, 1, 2, 3, ag0, 11))
    ag_drain(0)

    @pl.loop(0, Z)
    def _(zs):
        select(0, zs)

    run(ph_e1[0], e1_body, lambda i: at(i, 0, 2, 12, ag1, 0))

    @pl.loop(0, Z)
    def _(zs):
        gates(0, zs)

    run(ph_e2[0], e2_body(0), lambda i: at(i, 0, 2, 2, ag1, 12))
    for c in range(4):
        y_desc(0, c).wait_recv()

    @pl.loop(0, 4)
    def _(i):
        rs0(i)

    ag_drain(1)

    @pl.loop(0, Z)
    def _(zs):
        select(1, zs)
        gates(1, zs)

    run(ph_e1[1], e1_body, lambda i: at(i, 1, 4, 6, rs0, 4))
    run(ph_e2[1], e2_body(1), lambda i: at(i, 2, 3, 2, rs0, 10))
    for c in range(4):
        y_desc(1, c).wait_recv()

    @pl.loop(12, 14)
    def _(i):
        rs0(i)

    @pl.loop(0, 4)
    def _(i):
        rs1(i)

    run(ph_13b, w13_body(n13a))
    rs_final(0)
    run(ph_2, w2_body, lambda i: at(i, 0, 2, 4, rs1, 4))

    @pl.loop(8, 14)
    def _(i):
        rs1(i)

    rs_final(1)
    pl.when(k == 0)(lambda: m_desc(0).wait_recv())
    pl.when(k == 1)(lambda: m_desc(1).wait_recv())

    @pl.loop(0, 4)
    def _(c):
        own = cols(k * NCH + c)
        out[:, own] = (a[:, own].astype(F32) + f[:, own] + ms[k, c]).astype(BF)
        oth = cols(ok * NCH + c)
        out[:, oth] = (a[:, oth].astype(F32) + f[:, oth] + mr[c]).astype(BF)

    for p in range(2):
        @pl.when(k == p)
        def _():
            for c in own_descs(p):
                c.wait_send()
        pl.when(k != p)(lambda: m_desc(p).wait_send())
        for dirn in range(2):
            @pl.loop(0, 14)
            def _(i):
                ag_desc(p, dirn, i).wait_send()
                dd_desc(p, dirn, i).wait_send()
                rs_desc(p, dirn, i).wait_send()

            @pl.loop(0, NKG[dirn])
            def _(d):
                kg_desc(p, dirn, d).wait_send()

        @pl.loop(0, 4)
        def _(c):
            y_desc(p, c).wait_send()


def solution(mesh):
    G = mesh.shape['ep']

    def local(h0, idx, slot, na, wq, wk, wv, wo, nf, w1, w3, w2, nm, wr, ue1, ue3, ue2):
        b, s, d = h0.shape
        t = b * s
        kt = idx.shape[-1]
        el = ue1.shape[0]
        e = el * G
        cap = 2 * t * kt // e
        Z = G // 2
        nq, nk, ff, fe = wq.shape[1], wk.shape[1], w1.shape[1], ue1.shape[2]
        keyt = (idx * cap + slot).reshape(t, kt).T
        idxt = idx.reshape(t, kt).T
        pos = np.arange(s, dtype=np.float64)
        inv = ROPE_BASE ** (-2.0 * np.arange(HEAD // 2, dtype=np.float64) / HEAD)
        ang = pos[:, None] * inv[None, :]
        cosr = np.concatenate([np.cos(ang), np.cos(ang)], axis=1).astype(np.float32)
        sinr = np.concatenate([-np.sin(ang), np.sin(ang)], axis=1).astype(np.float32)
        nslot = el * cap
        rows = max(2 * d, nq, ff, el * fe)
        vm = pl.BlockSpec(memory_space=pltpu.VMEM)
        hb = pl.BlockSpec(memory_space=pl.ANY)
        V, DMA = pltpu.VMEM, pltpu.SemaphoreType.DMA
        kern = functools.partial(_kernel, Z, t, d, nq, nk, ff, el, fe, cap)
        out = pl.pallas_call(
            kern,
            out_shape=jax.ShapeDtypeStruct((t, d), BF),
            in_specs=[vm] * 9 + [hb] * 10,
            out_specs=vm,
            scratch_shapes=[
                V((2, Z, t // 16, 16, d), BF),
                V((2, Z, 16, t), F32),
                V((el, Z, cap, d), BF),
                V((el, Z * cap, fe), BF),
                V((2, 2, 4, Z, nslot, TN), BF),
                V((2, 4, Z, nslot, TN), BF),
                V((2, Z, 3 * t, 2 * nslot), BF),
                V((2, 2, 18, t, TN), F32),
                V((2, 4, t, TN), F32),
                V((4, t, TN), F32),
                V((NS, rows, TN), BF),
                V((t, d), BF),
                V((t, nq + 2 * nk), BF),
                V((t, nq), BF),
                V((t, d), BF),
                V((t, ff), BF),
                V((t, d), F32),
                DMA((NS, 8)),
                DMA((2,)), DMA((2,)),
                DMA((2, 2, 14)), DMA((2, 2, 14)),
                DMA((2, 2, 4)), DMA((2, 2, 4)),
                DMA((2, 2, 14)), DMA((2, 2, 14)),
                DMA((2, 4)), DMA((2, 4)),
                DMA((2, 2, 14)), DMA((2, 2, 14)),
                DMA((1,)), DMA((1,)),
            ],
            compiler_params=pltpu.CompilerParams(
                collective_id=0, has_side_effects=True, vmem_limit_bytes=VMEM_LIMIT),
            name="layer_pair",
        )(h0.reshape(t, d), keyt, idxt, na.reshape(1, d), nf.reshape(1, d), nm.reshape(1, d), wr,
          jnp.asarray(cosr), jnp.asarray(sinr), wq, wk, wv, wo, w1, w3, w2, ue1, ue3, ue2)
        return out.reshape(b, s, d)

    rows_spec = P(('dp', 'ep'))
    in_specs = (rows_spec,) * 3 + (P(),) * 11 + (P('ep'),) * 3
    return jax.shard_map(local, mesh=mesh, in_specs=in_specs, out_specs=rows_spec, check_vma=False)
```

```python
import functools

import jax
import jax.numpy as jnp
import numpy as np
from jax import lax
from jax.experimental import pallas as pl
from jax.experimental.pallas import tpu as pltpu
from jax.sharding import PartitionSpec as P

HEAD = 128
EPS = 1e-6
ROPE_BASE = 10000.0
TN = 256
NS = 4
VMEM_LIMIT = 66_500_000
MESH = pl.DeviceIdType.MESH
F32, BF = jnp.float32, jnp.bfloat16


def _rms_rows(xf, w):
    r = lax.rsqrt(jnp.mean(xf * xf, axis=-1, keepdims=True) + EPS)
    return (xf * r * w).astype(BF)


def _silu(x):
    return x * jax.nn.sigmoid(x)


def _div(x, n):
    return x // n if isinstance(x, int) else lax.div(x, n)


def _rem(x, n):
    return x % n if isinstance(x, int) else lax.rem(x, n)


def _dot(a, b):
    return jnp.dot(a, b, preferred_element_type=F32)


class Phase:
    def __init__(self, n, copies):
        self.n, self.copies, self.start = n, copies, 0


def _kernel(Z, T, D, NQ, NK, FF, EL, FE, CAP,
            h0, idx, slot, na, nf, nm, cosr, sinr, wr,
            wq, wk, wv, wo, w1, w3, w2, ue1, ue3, ue2,
            out,
            ubuf, kg, x, hid, ys, yr, g3, rb, ms, mr, wbuf, xn, qkv, o, a, fh, f, wrv,
            wsem, wr_sem, own_s, own_r, ag_s, ag_r, kg_s, kg_r, dd_s, dd_r, y_s, y_r, rs_s, rs_r, m_s, m_r):
    ep = lax.axis_index("ep")
    z = _div(ep, 2)
    k = _rem(ep, 2)
    ok = 1 - k
    RC = T // 16
    HC = RC // 2
    NC = D // TN
    NCH = NC // 2
    NM = 4 * HC - 2 if Z == 8 else None
    assert Z == 8 and HC == 4 and NCH == 4
    NSL = EL * CAP

    def dev(zz, kk):
        return {"ep": zz * 2 + kk}

    right, left = _rem(z + 1, Z), _rem(z + Z - 1, Z)
    nbr = (right, left)

    def rcopy(src, dst, s, r, zz, kk):
        return pltpu.make_async_remote_copy(src_ref=src, dst_ref=dst, send_sem=s, recv_sem=r,
                                            device_id=dev(zz, kk), device_id_type=MESH)

    def cols(i):
        return pl.ds(i * TN if isinstance(i, int) else pl.multiple_of(i * TN, TN), TN)

    def row(w):
        return w[...].astype(F32).reshape(1, D)

    def wslot(slot, lo, n):
        return wbuf.at[slot, pl.ds(lo, n)]

    nq2, nk2 = NQ // (2 * TN), NK // (2 * TN)

    def qkv_copies(i, slot):
        res = []
        for h in range(2):
            for cond, src, off in ((i < nq2, wq, 0), ((i >= nq2) & (i < nq2 + nk2), wk, nq2),
                                   (i >= nq2 + nk2, wv, nq2 + nk2)):
                res.append((cond, lambda src=src, off=off, h=h: pltpu.make_async_copy(
                    src.at[:, cols(2 * (i - off) + h)], wslot(slot, h * D, D), wsem.at[slot, h])))
        return res

    def wo_copies(i, slot):
        return [(None, lambda: pltpu.make_async_copy(wo.at[:, cols(i)], wslot(slot, 0, NQ), wsem.at[slot, 0]))]

    def w13_copies(i0):
        def go(i, slot):
            return [(None, lambda: pltpu.make_async_copy(w1.at[:, cols(i + i0)], wslot(slot, 0, D), wsem.at[slot, 0])),
                    (None, lambda: pltpu.make_async_copy(w3.at[:, cols(i + i0)], wslot(slot, D, D), wsem.at[slot, 1]))]
        return go

    def w2_copies(i, slot):
        return [(None, lambda: pltpu.make_async_copy(w2.at[:, cols(i)], wslot(slot, 0, FF), wsem.at[slot, 0]))]

    NJ = FE // TN

    def e1_copies(i, slot):
        e, j = _div(i, NJ), _rem(i, NJ)
        return [(None, lambda: pltpu.make_async_copy(ue1.at[e, :, cols(j)], wslot(slot, 0, D), wsem.at[slot, 0])),
                (None, lambda: pltpu.make_async_copy(ue3.at[e, :, cols(j)], wslot(slot, D, D), wsem.at[slot, 1]))]

    def e2_col(i):
        q = _div(i, 2)
        c = _rem(q, 2) * 2 + _div(q, 2)
        half = jnp.where(_rem(i, 2) == 0, ok, k)
        return half, c

    def e2_copies(i, slot):
        half, c = e2_col(i)
        return [(None, lambda e=e: pltpu.make_async_copy(
            ue2.at[e, :, cols(half * NCH + c)], wslot(slot, e * FE, FE), wsem.at[slot, e])) for e in range(EL)]

    n13 = FF // TN
    n13a = n13 // 4
    ph_qkv = Phase(nq2 + 2 * nk2, qkv_copies)
    ph_wo = Phase(D // TN, wo_copies)
    ph_13a = Phase(n13a, w13_copies(0))
    ph_e1 = [Phase(EL * NJ, e1_copies), Phase(EL * NJ, e1_copies)]
    ph_e2 = [Phase(NC, e2_copies), Phase(NC, e2_copies)]
    ph_13b = Phase(n13 - n13a, w13_copies(n13a))
    ph_2 = Phase(D // TN, w2_copies)
    order = [ph_qkv, ph_wo, ph_13a, ph_e1[0], ph_e2[0], ph_e1[1], ph_e2[1], ph_13b, ph_2]
    total = 0
    for q, ph in enumerate(order):
        ph.start, ph.pos = total, q
        total += ph.n

    def do(copies, act):
        for cond, mk in copies:
            if cond is None:
                act(mk())
            else:
                pl.when(cond)(lambda mk=mk: act(mk()))

    def issue(t, phases):
        slot = _rem(t, NS)
        for ph in phases:
            def go(ph=ph):
                do(ph.copies(t - ph.start, slot), lambda c: c.start())
            pl.when((t >= ph.start) & (t < ph.start + ph.n))(go)

    def run(ph, body, events=None):
        nxt = order[ph.pos:ph.pos + 2]

        def it(i, _):
            t = ph.start + i
            slot = _rem(t, NS)
            do(ph.copies(i, slot), lambda c: c.wait())
            body(i, slot)
            issue(t + NS, nxt)
            if events is not None:
                events(i)
            return 0

        lax.fori_loop(0, ph.n, it, 0)

    def at(i, start, stride, count, fn, e0):
        n = _div(i - start, stride)
        pl.when((i >= start) & (_rem(i - start, stride) == 0) & (n < count))(lambda: fn(e0 + n))

    def ag_desc(p, dirn, i):
        d = _div(i, 4)
        c = _rem(i + 2 * dirn, 4)
        org = _rem(z - d + Z, Z) if dirn == 0 else _rem(z + d, Z)
        blk = ubuf.at[p, org, k * HC + c]
        return rcopy(blk, blk, ag_s.at[p, dirn, i], ag_r.at[p, dirn, i], nbr[dirn], k)

    def kg_desc(p, dirn, d):
        org = _rem(z - d + Z, Z) if dirn == 0 else _rem(z + d, Z)
        blk = kg.at[p, org]
        return rcopy(blk, blk, kg_s.at[p, dirn, d], kg_r.at[p, dirn, d], nbr[dirn], k)

    def dd_desc(p, dirn, i):
        d = _div(i, 4) + 1
        c = _rem(i + 2 * dirn, 4)
        org = _rem(z - d + Z, Z) if dirn == 0 else _rem(z + d, Z)
        blk = ubuf.at[p, org, k * HC + c]
        return rcopy(blk, blk, dd_s.at[p, dirn, i], dd_r.at[p, dirn, i], z, ok)

    def own_desc(p, q):
        blk = (ubuf, kg)[q].at[p, z]
        return rcopy(blk, blk, own_s.at[q], own_r.at[q], z, ok)

    NKG = (4, 3)

    def ag_send_own(p):
        for i in range(4):
            for dirn in range(2):
                ag_desc(p, dirn, i).start()

    def kg_send_own(p):
        for dirn in range(2):
            kg_desc(p, dirn, 0).start()

    def ag_event(p):
        def ev(i):
            for dirn in range(2):
                ag_desc(p, dirn, i).wait_recv()
                pl.when(i < 10)(lambda: ag_desc(p, dirn, i + 4).start())
            for dirn in range(2):
                dd_desc(p, dirn, i).start()
            q = _div(i, 4)
            for dirn in range(2):
                @pl.when((_rem(i, 4) == 1) & (q < NKG[dirn]))
                def _():
                    kg_desc(p, dirn, q).wait_recv()
                    pl.when(q + 1 < NKG[dirn])(lambda: kg_desc(p, dirn, q + 1).start())
        return ev

    def dd_wait(p, dirn, i):
        blk = ubuf.at[p, 0, 0]
        rcopy(blk, blk, dd_s.at[p, dirn, i], dd_r.at[p, dirn, i], z, ok).wait_recv()

    def sel_step(p):
        def step(n):
            d, dirn = _div(n + 1, 2), _rem(n + 1, 2)

            @pl.when((n >= 1) & (n < 7))
            def _():
                @pl.loop(0, 4)
                def _(j):
                    dd_wait(p, dirn, 4 * (d - 1) + j)

            @pl.when(n == 7)
            def _():
                for j in (12, 13):
                    for q in range(2):
                        dd_wait(p, q, j)

            select(p, _rem(z + Z + jnp.where(dirn == 0, -d, d), Z))
        return step

    def key_hits(p, zs, j, base, n):
        keys = kg[p, zs, j:j + 1, :].astype(jnp.int32)
        return keys == base + lax.broadcasted_iota(jnp.int32, (n, T), 0)

    def select(p, zs):
        base = ep * NSL
        s = jnp.zeros((NSL, T), jnp.bool_)
        s = key_hits(p, zs, 0, base, NSL)
        for j in range(1, 8):
            s = s | key_hits(p, zs, j, base, NSL)
        s = jnp.where(s, 1.0, 0.0).astype(BF)
        for n in range(D // 512):
            u = ubuf[p, zs, :, :, n * 512:(n + 1) * 512].reshape(T, 512)
            xs = _dot(s, u).astype(BF)
            for e in range(EL):
                x[e, zs, :, n * 512:(n + 1) * 512] = xs[e * CAP:(e + 1) * CAP]

    def gates(p, zs):
        parts = []
        for kk in (k, ok):
            base = (z * 2 + kk) * NSL
            gt = jnp.zeros((NSL, T), F32)
            for j in range(8):
                gt = gt + jnp.where(key_hits(p, zs, j, base, NSL), kg[p, zs, 8 + j:9 + j, :], 0.0)
            parts.append(gt.T)
        for h, gt in enumerate(parts):
            hi = gt.astype(BF)
            r = gt - hi.astype(F32)
            mid = r.astype(BF)
            lo = (r - mid.astype(F32)).astype(BF)
            for q, v in enumerate((hi, mid, lo)):
                g3[p, zs, q * T:(q + 1) * T, h * NSL:(h + 1) * NSL] = v

    def combine(p, zd, c):
        yy = jnp.concatenate([ys[p, k, c, zd], yr[p, c, zd]], axis=0)
        r = _dot(g3[p, zd], yy)
        return r[:T] + (r[T:2 * T] + r[2 * T:])

    def rs_desc(p, dirn, i):
        return rcopy(rb.at[p, dirn, i], rb.at[p, dirn, i + 4], rs_s.at[p, dirn, i], rs_r.at[p, dirn, i],
                     nbr[dirn], k)

    def rs_event(p):
        def ev(i):
            j = i + 2
            d = 4 - _div(j, 4)
            for dirn in range(2):
                c = _rem(j + 2 - 2 * dirn, 4)
                zd = _rem(z + d, Z) if dirn == 0 else _rem(z - d + Z, Z)
                part = combine(p, zd, c)

                @pl.when(i >= 4)
                def _():
                    rs_desc(p, dirn, i - 4).wait_recv()
                    rb[p, dirn, i] = rb[p, dirn, i] + part

                @pl.when(i < 4)
                def _():
                    rb[p, dirn, i] = part
            for dirn in range(2):
                rs_desc(p, dirn, i).start()
        return ev

    def m_desc(p, c):
        return rcopy(ms.at[p, c], mr.at[c], m_s.at[c], m_r.at[c], z, ok)

    def rs_final(p):
        @pl.loop(0, 4)
        def _(c):
            ms[p, c] = combine(p, z, c)

        @pl.loop(0, 4)
        def _(s):
            c = _rem(s + 2, 4)
            rs_desc(p, 0, 10 + s).wait_recv()
            ms[p, c] = ms[p, c] + rb[p, 0, 14 + s]
            rs_desc(p, 1, 10 + s).wait_recv()
            ms[p, s] = ms[p, s] + rb[p, 1, 14 + s]

            @pl.when((s >= 2) & (k != p))
            def _():
                m_desc(p, c).start()
                m_desc(p, s).start()

    def y_desc(p, c):
        return rcopy(ys.at[p, ok, c], yr.at[p, c], y_s.at[p, c], y_r.at[p, c], z, ok)

    def qkv_body(i, slot):
        last = i >= nq2 + nk2
        cs = jnp.where(last, 1.0, cosr[...])
        sn = jnp.where(last, 0.0, sinr[...])
        for h in range(2):
            r = _dot(xn[...], wbuf[slot, h * D:(h + 1) * D])
            parts = []
            for b in range(TN // HEAD):
                v = r[:, b * HEAD:(b + 1) * HEAD]
                parts.append(v * cs + pltpu.roll(v, HEAD // 2, 1) * sn)
            qkv[:, cols(2 * i + h)] = jnp.concatenate(parts, axis=1).astype(BF)

    nkv = NK // HEAD
    rep = NQ // NK

    def attn(g):
        def hd(i):
            return pl.ds(pl.multiple_of(i * HEAD, HEAD), HEAD)
        kk = qkv[:, hd(NQ // HEAD + g)]
        vv = qkv[:, hd(NQ // HEAD + nkv + g)]
        causal = lax.broadcasted_iota(jnp.int32, (T, T), 0) >= lax.broadcasted_iota(jnp.int32, (T, T), 1)
        for hh in range(rep):
            qh = qkv[:, hd(g * rep + hh)]
            s = lax.dot_general(qh, kk, (((1,), (1,)), ((), ())), preferred_element_type=F32) * HEAD ** -0.5
            s = jnp.where(causal, s, -jnp.inf)
            e = jnp.exp(s - jnp.max(s, axis=-1, keepdims=True))
            pr = (e / jnp.sum(e, axis=-1, keepdims=True)).astype(BF)
            o[:, hd(g * rep + hh)] = _dot(pr, vv).astype(BF)

    def wo_body(i, slot):
        r = _dot(o[...], wbuf[slot, :NQ])
        a[:, cols(i)] = (h0[:, cols(i)].astype(F32) + r).astype(BF)

    def w13_body(i0):
        def body(i, slot):
            h1 = _dot(xn[...], wbuf[slot, :D])
            h3 = _dot(xn[...], wbuf[slot, D:2 * D])
            fh[:, cols(i + i0)] = (_silu(h1) * h3).astype(BF)
        return body

    def w2_body(i, slot):
        f[:, cols(i)] = _dot(fh[...], wbuf[slot, :FF])

    def e1_body(i, slot):
        e, j = _div(i, NJ), _rem(i, NJ)
        xe = x[e].reshape(Z * CAP, D)
        h1 = _dot(xe, wbuf[slot, :D])
        h3 = _dot(xe, wbuf[slot, D:2 * D])
        hid[e, :, cols(j)] = (_silu(h1) * h3).astype(BF)

    def e2_body(p, send=True):
        def body(i, slot):
            half, c = e2_col(i)
            for e in range(EL):
                r = _dot(hid[e], wbuf[slot, e * FE:(e + 1) * FE]).astype(BF)
                for zs in range(Z):
                    ys[p, half, c, zs, e * CAP:(e + 1) * CAP, :] = r[zs * CAP:(zs + 1) * CAP]
            if send:
                pl.when(_rem(i, 2) == 0)(lambda: y_desc(p, c).start())
        return body


    barrier = pltpu.get_barrier_semaphore()
    for zz, kk in ((right, k), (left, k), (z, ok)):
        pl.semaphore_signal(barrier, inc=1, device_id=dev(zz, kk), device_id_type=MESH)
    wr_copy = pltpu.make_async_copy(wr, wrv, wr_sem.at[0])
    wr_copy.start()
    for t in range(NS):
        issue(t, [ph_qkv])

    @pl.loop(0, RC)
    def _(r):
        rows = pl.ds(pl.multiple_of(r * 16, 16), 16)
        ubuf[k, z, r] = _rms_rows(h0[rows, :].astype(F32), row(nm))

    pl.semaphore_wait(barrier, 3)

    @pl.when(k == 0)
    def _():
        own_desc(0, 0).start()
        ag_send_own(0)

    @pl.when(k == 1)
    def _():
        own_desc(1, 0).start()

    wr_copy.wait()
    lt = _dot(ubuf[k, z].reshape(T, D), wrv[...]).T
    rows = []
    for j in range(8):
        hit = lax.broadcasted_iota(jnp.int32, lt.shape, 0) == idx[j:j + 1, :]
        rows.append(jnp.sum(jnp.where(hit, lt, 0.0), axis=0, keepdims=True))
    sel = jnp.concatenate(rows, axis=0)
    ex = jnp.exp(sel - jnp.max(sel, axis=0, keepdims=True))
    kg[k, z, 0:8, :] = (idx[...] * CAP + slot[...]).astype(F32)
    kg[k, z, 8:16, :] = ex / jnp.sum(ex, axis=0, keepdims=True)

    @pl.when(k == 1)
    def _():
        own_desc(0, 0).wait_recv()
        ag_send_own(0)

    for p in range(2):
        pl.when(k == p)(lambda: own_desc(p, 1).start())

    @pl.loop(0, RC)
    def _(r):
        rows = pl.ds(pl.multiple_of(r * 16, 16), 16)
        xn[rows, :] = _rms_rows(h0[rows, :].astype(F32), row(na))

    pl.when(k == 1)(lambda: own_desc(0, 1).wait_recv())
    kg_send_own(0)

    ag0, ag1 = ag_event(0), ag_event(1)
    rs0, rs1 = rs_event(0), rs_event(1)
    sel0, sel1 = sel_step(0), sel_step(1)

    run(ph_qkv, qkv_body, lambda i: at(i, 3, 2, 4, ag0, 0))

    @pl.loop(0, nkv)
    def _(g):
        attn(g)
        at(g, 0, 2, 2, ag0, 4)

    run(ph_wo, wo_body, lambda i: at(i, 0, 2, 4, ag0, 6))

    @pl.when(k == 0)
    def _():
        for q in range(2):
            own_desc(1, q).wait_recv()
    ag_send_own(1)
    kg_send_own(1)

    @pl.loop(0, RC)
    def _(r):
        rows = pl.ds(pl.multiple_of(r * 16, 16), 16)
        xn[rows, :] = _rms_rows(a[rows, :].astype(F32), row(nf))

    def ev_13a(i):
        at(i, 0, 2, 3, ag0, 10)
        at(i, 0, 1, 5, sel0, 0)
    run(ph_13a, w13_body(0), ev_13a)
    ag0(13)
    pl.loop(5, 8)(sel0)

    def ev_e10(i):
        at(i, 0, 2, 12, ag1, 0)
        at(i, 1, 2, 8, lambda n: gates(0, n), 0)
    run(ph_e1[0], e1_body, ev_e10)

    def rs_open(p, rs, half):
        for c in (half, half + 2):
            y_desc(p, c).wait_recv()
        pl.loop(0, 2)(lambda n: rs(2 * n + half))

    def ev_e20(i):
        at(i, 0, 1, 2, ag1, 12)
        pl.when(i == 4)(lambda: rs_open(0, rs0, 0))
    run(ph_e2[0], e2_body(0), ev_e20)
    rs_open(0, rs0, 1)
    pl.loop(0, 8)(sel1)
    rs0(4)

    def ev_e11(i):
        at(i, 2, 4, 6, rs0, 5)
        at(i, 1, 2, 8, lambda n: gates(1, n), 0)
    run(ph_e1[1], e1_body, ev_e11)

    def ev_e21(i):
        at(i, 1, 3, 2, rs0, 11)
        pl.when(i == 6)(lambda: rs_open(1, rs1, 0))
    run(ph_e2[1], e2_body(1), ev_e21)
    rs0(13)
    rs_open(1, rs1, 1)

    run(ph_13b, w13_body(n13a))
    rs_final(0)
    run(ph_2, w2_body, lambda i: at(i, 0, 3, 3, rs1, 4))
    pl.loop(7, 14)(rs1)
    rs_final(1)

    @pl.loop(0, 4)
    def _(c):
        own = cols(k * NCH + c)
        out[:, own] = (a[:, own].astype(F32) + f[:, own] + ms[k, c]).astype(BF)

    @pl.loop(0, 4)
    def _(n):
        c = _rem(n, 2) * 2 + _div(n, 2)
        m_desc(0, c).wait_recv()
        oth = cols(ok * NCH + c)
        out[:, oth] = (a[:, oth].astype(F32) + f[:, oth] + mr[c]).astype(BF)

    for p in range(2):
        @pl.when(k == p)
        def _():
            for q in range(2):
                own_desc(p, q).wait_send()

        @pl.when(k != p)
        def _():
            for c in range(4):
                m_desc(p, c).wait_send()

        for dirn in range(2):
            @pl.loop(0, 14)
            def _(i):
                ag_desc(p, dirn, i).wait_send()
                dd_desc(p, dirn, i).wait_send()
                rs_desc(p, dirn, i).wait_send()

            @pl.loop(0, NKG[dirn])
            def _(d):
                kg_desc(p, dirn, d).wait_send()

        @pl.loop(0, 4)
        def _(c):
            y_desc(p, c).wait_send()


def solution(mesh):
    G = mesh.shape['ep']

    def local(h0, idx, slot, na, wq, wk, wv, wo, nf, w1, w3, w2, nm, wr, ue1, ue3, ue2):
        b, s, d = h0.shape
        t = b * s
        kt = idx.shape[-1]
        el = ue1.shape[0]
        e = el * G
        cap = 2 * t * kt // e
        Z = G // 2
        nq, nk, ff, fe = wq.shape[1], wk.shape[1], w1.shape[1], ue1.shape[2]
        pos = np.arange(s, dtype=np.float64)
        inv = ROPE_BASE ** (-2.0 * np.arange(HEAD // 2, dtype=np.float64) / HEAD)
        ang = pos[:, None] * inv[None, :]
        cosr = np.concatenate([np.cos(ang), np.cos(ang)], axis=1).astype(np.float32)
        sinr = np.concatenate([-np.sin(ang), np.sin(ang)], axis=1).astype(np.float32)
        nslot = el * cap
        rows = max(2 * d, nq, ff, el * fe)
        vm = pl.BlockSpec(memory_space=pltpu.VMEM)
        hb = pl.BlockSpec(memory_space=pl.ANY)
        V, DMA = pltpu.VMEM, pltpu.SemaphoreType.DMA
        operands = (h0.reshape(t, d), idx.reshape(t, kt).T, slot.reshape(t, kt).T, na, nf, nm,
                    jnp.asarray(cosr), jnp.asarray(sinr), wr, wq, wk, wv, wo, w1, w3, w2, ue1, ue3, ue2)

        def call(cid):
            kern = functools.partial(_kernel, Z, t, d, nq, nk, ff, el, fe, cap)
            return pl.pallas_call(
                kern,
                out_shape=jax.ShapeDtypeStruct((t, d), BF),
                in_specs=[vm] * 8 + [hb] * 11,
                out_specs=vm,
                scratch_shapes=[
                    V((2, Z, t // 16, 16, d), BF),
                    V((2, Z, 16, t), F32),
                    V((el, Z, cap, d), BF),
                    V((el, Z * cap, fe), BF),
                    V((2, 2, 4, Z, nslot, TN), BF),
                    V((2, 4, Z, nslot, TN), BF),
                    V((2, Z, 3 * t, 2 * nslot), BF),
                    V((2, 2, 18, t, TN), F32),
                    V((2, 4, t, TN), F32),
                    V((4, t, TN), F32),
                    V((NS, rows, TN), BF),
                    V((t, d), BF),
                    V((t, nq + 2 * nk), BF),
                    V((t, nq), BF),
                    V((t, d), BF),
                    V((t, ff), BF),
                    V((t, d), F32),
                    V((d, e), BF),
                    DMA((NS, 8)), DMA((1,)),
                    DMA((2,)), DMA((2,)),
                    DMA((2, 2, 14)), DMA((2, 2, 14)),
                    DMA((2, 2, 4)), DMA((2, 2, 4)),
                    DMA((2, 2, 14)), DMA((2, 2, 14)),
                    DMA((2, 4)), DMA((2, 4)),
                    DMA((2, 2, 14)), DMA((2, 2, 14)),
                    DMA((4,)), DMA((4,)),
                ],
                compiler_params=pltpu.CompilerParams(
                    collective_id=cid, has_side_effects=True, vmem_limit_bytes=VMEM_LIMIT),
                name="layer_pair",
            )(*operands)

        out = call(0)
        return out.reshape(b, s, d)

    rows_spec = P(('dp', 'ep'))
    in_specs = (rows_spec,) * 3 + (P(),) * 11 + (P('ep'),) * 3
    return jax.shard_map(local, mesh=mesh, in_specs=in_specs, out_specs=rows_spec, check_vma=False)
```

```python
import functools

import jax
import jax.numpy as jnp
import numpy as np
from jax import lax
from jax.experimental import pallas as pl
from jax.experimental.pallas import tpu as pltpu
from jax.sharding import PartitionSpec as P

HEAD = 128
EPS = 1e-6
ROPE_BASE = 10000.0
TN = 256
NS = 4
VMEM_LIMIT = 66_500_000
MESH = pl.DeviceIdType.MESH
F32, BF = jnp.float32, jnp.bfloat16


def _rms_rows(xf, w):
    r = lax.rsqrt(jnp.mean(xf * xf, axis=-1, keepdims=True) + EPS)
    return (xf * r * w).astype(BF)


def _silu(x):
    return x * jax.nn.sigmoid(x)


def _div(x, n):
    return x // n if isinstance(x, int) else lax.div(x, n)


def _rem(x, n):
    return x % n if isinstance(x, int) else lax.rem(x, n)


def _dot(a, b):
    return jnp.dot(a, b, preferred_element_type=F32)


class Phase:
    def __init__(self, n, copies):
        self.n, self.copies, self.start = n, copies, 0


def _kernel(Z, T, D, NQ, NK, FF, EL, FE, CAP,
            h0, idx, slot, na, nf, nm, cosr, sinr, wr,
            wq, wk, wv, wo, w1, w3, w2, ue1, ue3, ue2,
            out,
            ubuf, kg, x, hid, ys, yr, g3, rb, ms, mr, wbuf, xn, qkv, o, a, fh, f, wrv,
            wsem, wr_sem, own_s, own_r, ag_s, ag_r, kg_s, kg_r, dd_s, dd_r, y_s, y_r, rs_s, rs_r, m_s, m_r):
    ep = lax.axis_index("ep")
    z = _div(ep, 2)
    k = _rem(ep, 2)
    ok = 1 - k
    RC = T // 16
    HC = RC // 2
    NC = D // TN
    NCH = NC // 2
    NM = 4 * HC - 2 if Z == 8 else None
    assert Z == 8 and HC == 4 and NCH == 4
    NSL = EL * CAP

    def dev(zz, kk):
        return {"ep": zz * 2 + kk}

    right, left = _rem(z + 1, Z), _rem(z + Z - 1, Z)
    nbr = (right, left)

    def rcopy(src, dst, s, r, zz, kk):
        return pltpu.make_async_remote_copy(src_ref=src, dst_ref=dst, send_sem=s, recv_sem=r,
                                            device_id=dev(zz, kk), device_id_type=MESH)

    def cols(i):
        return pl.ds(i * TN if isinstance(i, int) else pl.multiple_of(i * TN, TN), TN)

    def row(w):
        return w[...].astype(F32).reshape(1, D)

    def wslot(slot, lo, n):
        return wbuf.at[slot, pl.ds(lo, n)]

    nq2, nk2 = NQ // (2 * TN), NK // (2 * TN)

    def qkv_copies(i, slot):
        res = []
        for h in range(2):
            for cond, src, off in ((i < nq2, wq, 0), ((i >= nq2) & (i < nq2 + nk2), wk, nq2),
                                   (i >= nq2 + nk2, wv, nq2 + nk2)):
                res.append((cond, lambda src=src, off=off, h=h: pltpu.make_async_copy(
                    src.at[:, cols(2 * (i - off) + h)], wslot(slot, h * D, D), wsem.at[slot, h])))
        return res

    def wo_copies(i, slot):
        return [(None, lambda: pltpu.make_async_copy(wo.at[:, cols(i)], wslot(slot, 0, NQ), wsem.at[slot, 0]))]

    def w13_copies(i, slot):
        return [(None, lambda: pltpu.make_async_copy(w1.at[:, cols(i)], wslot(slot, 0, D), wsem.at[slot, 0])),
                (None, lambda: pltpu.make_async_copy(w3.at[:, cols(i)], wslot(slot, D, D), wsem.at[slot, 1]))]

    def w2_copies(i, slot):
        return [(None, lambda: pltpu.make_async_copy(w2.at[:, cols(i)], wslot(slot, 0, FF), wsem.at[slot, 0]))]

    NJ = FE // TN

    def e1_copies(i, slot):
        e, j = _div(i, NJ), _rem(i, NJ)
        return [(None, lambda: pltpu.make_async_copy(ue1.at[e, :, cols(j)], wslot(slot, 0, D), wsem.at[slot, 0])),
                (None, lambda: pltpu.make_async_copy(ue3.at[e, :, cols(j)], wslot(slot, D, D), wsem.at[slot, 1]))]

    def e2_col(i):
        q = _div(i, 2)
        c = _rem(q, 2) * 2 + _div(q, 2)
        half = jnp.where(_rem(i, 2) == 0, ok, k)
        return half, c

    def e2_copies(i, slot):
        half, c = e2_col(i)
        return [(None, lambda e=e: pltpu.make_async_copy(
            ue2.at[e, :, cols(half * NCH + c)], wslot(slot, e * FE, FE), wsem.at[slot, e])) for e in range(EL)]

    n13 = FF // TN
    ph_qkv = Phase(nq2 + 2 * nk2, qkv_copies)
    ph_wo = Phase(D // TN, wo_copies)
    ph_e1 = [Phase(EL * NJ, e1_copies), Phase(EL * NJ, e1_copies)]
    ph_e2 = [Phase(NC, e2_copies), Phase(NC, e2_copies)]
    ph_13 = Phase(n13, w13_copies)
    ph_2 = Phase(D // TN, w2_copies)
    order = [ph_qkv, ph_wo, ph_e1[0], ph_e2[0], ph_e1[1], ph_e2[1], ph_13, ph_2]
    total = 0
    for q, ph in enumerate(order):
        ph.start, ph.pos = total, q
        total += ph.n

    def do(copies, act):
        for cond, mk in copies:
            if cond is None:
                act(mk())
            else:
                pl.when(cond)(lambda mk=mk: act(mk()))

    def issue(t, phases):
        slot = _rem(t, NS)
        for ph in phases:
            def go(ph=ph):
                do(ph.copies(t - ph.start, slot), lambda c: c.start())
            pl.when((t >= ph.start) & (t < ph.start + ph.n))(go)

    def run(ph, body, events=None):
        nxt = order[ph.pos:ph.pos + 2]

        def it(i, _):
            t = ph.start + i
            slot = _rem(t, NS)
            do(ph.copies(i, slot), lambda c: c.wait())
            body(i, slot)
            issue(t + NS, nxt)
            if events is not None:
                events(i)
            return 0

        lax.fori_loop(0, ph.n, it, 0)

    def at(i, start, stride, count, fn, e0):
        n = _div(i - start, stride)
        pl.when((i >= start) & (_rem(i - start, stride) == 0) & (n < count))(lambda: fn(e0 + n))

    def ag_desc(p, dirn, i):
        d = _div(i, 4)
        c = _rem(i + 2 * dirn, 4)
        org = _rem(z - d + Z, Z) if dirn == 0 else _rem(z + d, Z)
        blk = ubuf.at[p, org, k * HC + c]
        return rcopy(blk, blk, ag_s.at[p, dirn, i], ag_r.at[p, dirn, i], nbr[dirn], k)

    def kg_desc(p, dirn, d):
        org = _rem(z - d + Z, Z) if dirn == 0 else _rem(z + d, Z)
        blk = kg.at[p, org]
        return rcopy(blk, blk, kg_s.at[p, dirn, d], kg_r.at[p, dirn, d], nbr[dirn], k)

    def dd_desc(p, dirn, i):
        d = _div(i, 4) + 1
        c = _rem(i + 2 * dirn, 4)
        org = _rem(z - d + Z, Z) if dirn == 0 else _rem(z + d, Z)
        blk = ubuf.at[p, org, k * HC + c]
        return rcopy(blk, blk, dd_s.at[p, dirn, i], dd_r.at[p, dirn, i], z, ok)

    def own_desc(p, q):
        blk = (ubuf, kg)[q].at[p, z]
        return rcopy(blk, blk, own_s.at[q], own_r.at[q], z, ok)

    NKG = (4, 3)

    def ag_send_own(p, half):
        for i in (2 * half, 2 * half + 1):
            for dirn in range(2):
                ag_desc(p, dirn, i).start()

    def kg_send_own(p):
        for dirn in range(2):
            kg_desc(p, dirn, 0).start()

    def ag_event(p):
        def ev(i):
            for dirn in range(2):
                ag_desc(p, dirn, i).wait_recv()
                pl.when(i < 10)(lambda: ag_desc(p, dirn, i + 4).start())
            for dirn in range(2):
                dd_desc(p, dirn, i).start()
            q = _div(i, 4)
            for dirn in range(2):
                @pl.when((_rem(i, 4) == 1) & (q < NKG[dirn]))
                def _():
                    kg_desc(p, dirn, q).wait_recv()
                    pl.when(q + 1 < NKG[dirn])(lambda: kg_desc(p, dirn, q + 1).start())
        return ev

    def ag_pair(p):
        ev = ag_event(p)

        def pair(n):
            pl.loop(0, 2)(lambda q: ev(2 * n + q))
        return pair

    def dd_wait(p, dirn, i):
        blk = ubuf.at[p, 0, 0]
        rcopy(blk, blk, dd_s.at[p, dirn, i], dd_r.at[p, dirn, i], z, ok).wait_recv()

    def sel_step(p):
        def step(n):
            d, dirn = _div(n + 1, 2), _rem(n + 1, 2)

            @pl.when((n >= 1) & (n < 7))
            def _():
                @pl.loop(0, 4)
                def _(j):
                    dd_wait(p, dirn, 4 * (d - 1) + j)

            @pl.when(n == 7)
            def _():
                for j in (12, 13):
                    for q in range(2):
                        dd_wait(p, q, j)

            select(p, _rem(z + Z + jnp.where(dirn == 0, -d, d), Z))
        return step

    def key_hits(p, zs, j, base, n):
        keys = kg[p, zs, j:j + 1, :].astype(jnp.int32)
        return keys == base + lax.broadcasted_iota(jnp.int32, (n, T), 0)

    def select(p, zs):
        base = ep * NSL
        s = jnp.zeros((NSL, T), jnp.bool_)
        s = key_hits(p, zs, 0, base, NSL)
        for j in range(1, 8):
            s = s | key_hits(p, zs, j, base, NSL)
        s = jnp.where(s, 1.0, 0.0).astype(BF)
        for n in range(D // 512):
            u = ubuf[p, zs, :, :, n * 512:(n + 1) * 512].reshape(T, 512)
            xs = _dot(s, u).astype(BF)
            for e in range(EL):
                x[e, zs, :, n * 512:(n + 1) * 512] = xs[e * CAP:(e + 1) * CAP]

    def gates(p, zs):
        parts = []
        for kk in (k, ok):
            base = (z * 2 + kk) * NSL
            gt = jnp.zeros((NSL, T), F32)
            for j in range(8):
                gt = gt + jnp.where(key_hits(p, zs, j, base, NSL), kg[p, zs, 8 + j:9 + j, :], 0.0)
            parts.append(gt.T)
        for h, gt in enumerate(parts):
            hi = gt.astype(BF)
            r = gt - hi.astype(F32)
            mid = r.astype(BF)
            lo = (r - mid.astype(F32)).astype(BF)
            for q, v in enumerate((hi, mid, lo)):
                g3[p, zs, q * T:(q + 1) * T, h * NSL:(h + 1) * NSL] = v

    def combine(p, zd, c):
        yy = jnp.concatenate([ys[p, k, c, zd], yr[p, c, zd]], axis=0)
        r = _dot(g3[p, zd], yy)
        return r[:T] + (r[T:2 * T] + r[2 * T:])

    def rs_desc(p, dirn, i):
        return rcopy(rb.at[p, dirn, i], rb.at[p, dirn, i + 4], rs_s.at[p, dirn, i], rs_r.at[p, dirn, i],
                     nbr[dirn], k)

    def rs_event(p):
        def ev(n):
            r = _rem(n, 4)
            i = jnp.where((r == 1) & (n < 12), n + 1, jnp.where((r == 2) & (n < 12), n - 1, n))
            j = i + 2
            d = 4 - _div(j, 4)
            for dirn in range(2):
                c = _rem(j + 2 - 2 * dirn, 4)
                zd = _rem(z + d, Z) if dirn == 0 else _rem(z - d + Z, Z)
                part = combine(p, zd, c)

                @pl.when(i >= 4)
                def _():
                    rs_desc(p, dirn, i - 4).wait_recv()
                    rb[p, dirn, i] = rb[p, dirn, i] + part

                @pl.when(i < 4)
                def _():
                    rb[p, dirn, i] = part
            for dirn in range(2):
                rs_desc(p, dirn, i).start()
        return ev

    def m_desc(p, c):
        return rcopy(ms.at[p, c], mr.at[c], m_s.at[c], m_r.at[c], z, ok)

    def rs_final(p):
        @pl.loop(0, 4)
        def _(c):
            ms[p, c] = combine(p, z, c)

        @pl.loop(0, 4)
        def _(s):
            c = _rem(s + 2, 4)
            rs_desc(p, 0, 10 + s).wait_recv()
            ms[p, c] = ms[p, c] + rb[p, 0, 14 + s]
            rs_desc(p, 1, 10 + s).wait_recv()
            ms[p, s] = ms[p, s] + rb[p, 1, 14 + s]

            @pl.when((s >= 2) & (k != p))
            def _():
                m_desc(p, c).start()
                m_desc(p, s).start()

    def y_desc(p, c):
        return rcopy(ys.at[p, ok, c], yr.at[p, c], y_s.at[p, c], y_r.at[p, c], z, ok)

    def qkv_body(i, slot):
        last = i >= nq2 + nk2
        cs = jnp.where(last, 1.0, cosr[...])
        sn = jnp.where(last, 0.0, sinr[...])
        for h in range(2):
            r = _dot(xn[...], wbuf[slot, h * D:(h + 1) * D])
            parts = []
            for b in range(TN // HEAD):
                v = r[:, b * HEAD:(b + 1) * HEAD]
                parts.append(v * cs + pltpu.roll(v, HEAD // 2, 1) * sn)
            qkv[:, cols(2 * i + h)] = jnp.concatenate(parts, axis=1).astype(BF)

    nkv = NK // HEAD
    rep = NQ // NK

    def attn(g):
        def hd(i):
            return pl.ds(pl.multiple_of(i * HEAD, HEAD), HEAD)
        kk = qkv[:, hd(NQ // HEAD + g)]
        vv = qkv[:, hd(NQ // HEAD + nkv + g)]
        causal = lax.broadcasted_iota(jnp.int32, (T, T), 0) >= lax.broadcasted_iota(jnp.int32, (T, T), 1)
        for hh in range(rep):
            qh = qkv[:, hd(g * rep + hh)]
            s = lax.dot_general(qh, kk, (((1,), (1,)), ((), ())), preferred_element_type=F32) * HEAD ** -0.5
            s = jnp.where(causal, s, -jnp.inf)
            e = jnp.exp(s - jnp.max(s, axis=-1, keepdims=True))
            pr = (e / jnp.sum(e, axis=-1, keepdims=True)).astype(BF)
            o[:, hd(g * rep + hh)] = _dot(pr, vv).astype(BF)

    def wo_body(i, slot):
        r = _dot(o[...], wbuf[slot, :NQ])
        a[:, cols(i)] = (h0[:, cols(i)].astype(F32) + r).astype(BF)

    def w13_body(i, slot):
        h1 = _dot(xn[...], wbuf[slot, :D])
        h3 = _dot(xn[...], wbuf[slot, D:2 * D])
        fh[:, cols(i)] = (_silu(h1) * h3).astype(BF)

    def w2_body(i, slot):
        f[:, cols(i)] = _dot(fh[...], wbuf[slot, :FF])

    def e1_body(i, slot):
        e, j = _div(i, NJ), _rem(i, NJ)
        xe = x[e].reshape(Z * CAP, D)
        h1 = _dot(xe, wbuf[slot, :D])
        h3 = _dot(xe, wbuf[slot, D:2 * D])
        hid[e, :, cols(j)] = (_silu(h1) * h3).astype(BF)

    def e2_body(p, send=True):
        def body(i, slot):
            half, c = e2_col(i)
            for e in range(EL):
                r = _dot(hid[e], wbuf[slot, e * FE:(e + 1) * FE]).astype(BF)
                for zs in range(Z):
                    ys[p, half, c, zs, e * CAP:(e + 1) * CAP, :] = r[zs * CAP:(zs + 1) * CAP]
            if send:
                pl.when(_rem(i, 2) == 0)(lambda: y_desc(p, c).start())
        return body


    barrier = pltpu.get_barrier_semaphore()
    for zz, kk in ((right, k), (left, k), (z, ok)):
        pl.semaphore_signal(barrier, inc=1, device_id=dev(zz, kk), device_id_type=MESH)
    wr_copy = pltpu.make_async_copy(wr, wrv, wr_sem.at[0])
    wr_copy.start()
    for t in range(NS):
        issue(t, [ph_qkv])

    @pl.loop(0, RC)
    def _(r):
        rows = pl.ds(pl.multiple_of(r * 16, 16), 16)
        ubuf[k, z, r] = _rms_rows(h0[rows, :].astype(F32), row(nm))

    pl.semaphore_wait(barrier, 3)

    @pl.when(k == 0)
    def _():
        own_desc(0, 0).start()
        ag_send_own(0, 0)

    @pl.when(k == 1)
    def _():
        own_desc(1, 0).start()

    wr_copy.wait()
    lt = _dot(ubuf[k, z].reshape(T, D), wrv[...]).T
    rows = []
    for j in range(8):
        hit = lax.broadcasted_iota(jnp.int32, lt.shape, 0) == idx[j:j + 1, :]
        rows.append(jnp.sum(jnp.where(hit, lt, 0.0), axis=0, keepdims=True))
    sel = jnp.concatenate(rows, axis=0)
    ex = jnp.exp(sel - jnp.max(sel, axis=0, keepdims=True))
    kg[k, z, 0:8, :] = (idx[...] * CAP + slot[...]).astype(F32)
    kg[k, z, 8:16, :] = ex / jnp.sum(ex, axis=0, keepdims=True)

    pl.when(k == 0)(lambda: ag_send_own(0, 1))

    @pl.when(k == 1)
    def _():
        own_desc(0, 0).wait_recv()
        ag_send_own(0, 0)

    for p in range(2):
        pl.when(k == p)(lambda: own_desc(p, 1).start())

    @pl.loop(0, RC)
    def _(r):
        rows = pl.ds(pl.multiple_of(r * 16, 16), 16)
        xn[rows, :] = _rms_rows(h0[rows, :].astype(F32), row(na))

    pl.when(k == 1)(lambda: own_desc(0, 1).wait_recv())
    kg_send_own(0)

    ag0, ag1 = ag_pair(0), ag_pair(1)
    rs0, rs1 = rs_event(0), rs_event(1)
    sel0, sel1 = sel_step(0), sel_step(1)

    def ev_qkv(i):
        pl.when((i == 1) & (k == 1))(lambda: ag_send_own(0, 1))
        at(i, 3, 4, 2, ag0, 0)
    run(ph_qkv, qkv_body, ev_qkv)

    @pl.loop(0, nkv)
    def _(g):
        attn(g)
        at(g, 1, 2, 1, ag0, 2)

    def ev_wo(i):
        at(i, 1, 4, 2, ag0, 3)
        at(i, 2, 1, 3, sel0, 0)
    run(ph_wo, wo_body, ev_wo)

    @pl.when(k == 0)
    def _():
        for q in range(2):
            own_desc(1, q).wait_recv()
    pl.loop(3, 5)(sel0)

    @pl.loop(0, RC)
    def _(r):
        rows = pl.ds(pl.multiple_of(r * 16, 16), 16)
        xn[rows, :] = _rms_rows(a[rows, :].astype(F32), row(nf))

    ag0(5)
    pl.loop(5, 7)(sel0)
    ag0(6)
    ag_send_own(1, 0)
    kg_send_own(1)
    sel0(7)

    def ev_e10(i):
        pl.when(i == 1)(lambda: ag_send_own(1, 1))
        at(i, 4, 4, 5, ag1, 0)
        at(i, 1, 2, 8, lambda n: gates(0, n), 0)
    run(ph_e1[0], e1_body, ev_e10)

    def rs_open(p, rs, half):
        for c in (half, half + 2):
            y_desc(p, c).wait_recv()
        pl.loop(2 * half, 2 * half + 2)(rs)

    def ev_e20(i):
        pl.when(i == 0)(lambda: ag1(5))
        pl.when(i == 4)(lambda: rs_open(0, rs0, 0))
    run(ph_e2[0], e2_body(0), ev_e20)
    rs_open(0, rs0, 1)
    ag1(6)
    pl.loop(0, 8)(sel1)
    rs0(4)

    def ev_e11(i):
        at(i, 2, 4, 6, rs0, 5)
        at(i, 1, 2, 8, lambda n: gates(1, n), 0)
    run(ph_e1[1], e1_body, ev_e11)

    def ev_e21(i):
        at(i, 1, 3, 2, rs0, 11)
        pl.when(i == 6)(lambda: rs_open(1, rs1, 0))
    run(ph_e2[1], e2_body(1), ev_e21)
    rs0(13)
    rs_open(1, rs1, 1)

    run(ph_13, w13_body, lambda i: at(i, 18, 4, 2, rs1, 4))
    rs_final(0)
    run(ph_2, w2_body, lambda i: at(i, 0, 3, 3, rs1, 6))
    pl.loop(9, 14)(rs1)
    rs_final(1)

    @pl.loop(0, 4)
    def _(c):
        own = cols(k * NCH + c)
        out[:, own] = (a[:, own].astype(F32) + f[:, own] + ms[k, c]).astype(BF)

    @pl.loop(0, 4)
    def _(n):
        c = _rem(n, 2) * 2 + _div(n, 2)
        m_desc(0, c).wait_recv()
        oth = cols(ok * NCH + c)
        out[:, oth] = (a[:, oth].astype(F32) + f[:, oth] + mr[c]).astype(BF)

    for p in range(2):
        @pl.when(k == p)
        def _():
            for q in range(2):
                own_desc(p, q).wait_send()

        @pl.when(k != p)
        def _():
            for c in range(4):
                m_desc(p, c).wait_send()

        for dirn in range(2):
            @pl.loop(0, 14)
            def _(i):
                ag_desc(p, dirn, i).wait_send()
                dd_desc(p, dirn, i).wait_send()
                rs_desc(p, dirn, i).wait_send()

            @pl.loop(0, NKG[dirn])
            def _(d):
                kg_desc(p, dirn, d).wait_send()

        @pl.loop(0, 4)
        def _(c):
            y_desc(p, c).wait_send()


def solution(mesh):
    G = mesh.shape['ep']

    def local(h0, idx, slot, na, wq, wk, wv, wo, nf, w1, w3, w2, nm, wr, ue1, ue3, ue2):
        b, s, d = h0.shape
        t = b * s
        kt = idx.shape[-1]
        el = ue1.shape[0]
        e = el * G
        cap = 2 * t * kt // e
        Z = G // 2
        nq, nk, ff, fe = wq.shape[1], wk.shape[1], w1.shape[1], ue1.shape[2]
        pos = np.arange(s, dtype=np.float64)
        inv = ROPE_BASE ** (-2.0 * np.arange(HEAD // 2, dtype=np.float64) / HEAD)
        ang = pos[:, None] * inv[None, :]
        cosr = np.concatenate([np.cos(ang), np.cos(ang)], axis=1).astype(np.float32)
        sinr = np.concatenate([-np.sin(ang), np.sin(ang)], axis=1).astype(np.float32)
        nslot = el * cap
        rows = max(2 * d, nq, ff, el * fe)
        vm = pl.BlockSpec(memory_space=pltpu.VMEM)
        hb = pl.BlockSpec(memory_space=pl.ANY)
        V, DMA = pltpu.VMEM, pltpu.SemaphoreType.DMA
        operands = (h0.reshape(t, d), idx.reshape(t, kt).T, slot.reshape(t, kt).T, na, nf, nm,
                    jnp.asarray(cosr), jnp.asarray(sinr), wr, wq, wk, wv, wo, w1, w3, w2, ue1, ue3, ue2)

        def call(cid):
            kern = functools.partial(_kernel, Z, t, d, nq, nk, ff, el, fe, cap)
            return pl.pallas_call(
                kern,
                out_shape=jax.ShapeDtypeStruct((t, d), BF),
                in_specs=[vm] * 8 + [hb] * 11,
                out_specs=vm,
                scratch_shapes=[
                    V((2, Z, t // 16, 16, d), BF),
                    V((2, Z, 16, t), F32),
                    V((el, Z, cap, d), BF),
                    V((el, Z * cap, fe), BF),
                    V((2, 2, 4, Z, nslot, TN), BF),
                    V((2, 4, Z, nslot, TN), BF),
                    V((2, Z, 3 * t, 2 * nslot), BF),
                    V((2, 2, 18, t, TN), F32),
                    V((2, 4, t, TN), F32),
                    V((4, t, TN), F32),
                    V((NS, rows, TN), BF),
                    V((t, d), BF),
                    V((t, nq + 2 * nk), BF),
                    V((t, nq), BF),
                    V((t, d), BF),
                    V((t, ff), BF),
                    V((t, d), F32),
                    V((d, e), BF),
                    DMA((NS, 8)), DMA((1,)),
                    DMA((2,)), DMA((2,)),
                    DMA((2, 2, 14)), DMA((2, 2, 14)),
                    DMA((2, 2, 4)), DMA((2, 2, 4)),
                    DMA((2, 2, 14)), DMA((2, 2, 14)),
                    DMA((2, 4)), DMA((2, 4)),
                    DMA((2, 2, 14)), DMA((2, 2, 14)),
                    DMA((4,)), DMA((4,)),
                ],
                compiler_params=pltpu.CompilerParams(
                    collective_id=cid, has_side_effects=True, vmem_limit_bytes=VMEM_LIMIT),
                name="layer_pair",
            )(*operands)

        out = call(0)
        return out.reshape(b, s, d)

    rows_spec = P(('dp', 'ep'))
    in_specs = (rows_spec,) * 3 + (P(),) * 11 + (P('ep'),) * 3
    return jax.shard_map(local, mesh=mesh, in_specs=in_specs, out_specs=rows_spec, check_vma=False)
```
